128 devices in a mesh: dp: 32 (over y, z, core), fsdp: 4 (over x).
Axes of the slice: x: 4, y: 4, z: 4, core: 2. Of those that a mesh axis runs over, the one named last changes fastest.
Arguments:
- tokens: bfloat16 [65536, 4096], P(('dp', 'fsdp')), may hold values from -0.75 to 0.75
- doc_ids: int32 [65536], P(('dp', 'fsdp')), may hold values from 0 to 63, never falling along the last dimension, each value on 1 to 2048 neighbouring positions
- attn_gain: float32 [4096], replicated, may hold values from 0.1 to 1.9
- mlp_gain: float32 [4096], replicated, may hold values from 0.1 to 1.9
- w_query: bfloat16 [4096, 512], P(('dp', 'fsdp')), may hold values from -1 to 1
- w_key_value: bfloat16 [4096, 256], P(('dp', 'fsdp')), may hold values from -3 to 3
- w_out: bfloat16 [512, 4096], P(None, ('dp', 'fsdp')), may hold values from -0.25 to 0.25
- w_gate: bfloat16 [4096, 1024], P(('dp', 'fsdp')), may hold values from -0.09375 to 0.09375
- w_up: bfloat16 [4096, 1024], P(('dp', 'fsdp')), may hold values from -0.09375 to 0.09375
- w_down: bfloat16 [1024, 4096], P(None, ('dp', 'fsdp')), may hold values from -0.1875 to 0.1875
Outputs:
- mixed: bfloat16 [65536, 4096], P(('dp', 'fsdp'))
The draws below stay inside these ranges and needn't reach their ends.
Inputs may be any that keep to these rules, and one draw needn't show every extreme that they name: `doc_ids`: document numbers never fall along the pack, and every document has at most 2048 tokens.
All inputs are finite; a program needn't handle non-finite values.
Results may differ from the reference program's by a relative error of at most 0.02.
The reference program's roundings to bfloat16 on the way count: a program that leaves them out, or rounds other values in their place, can miss the bound.
Values may be sent and summed in bfloat16 or wider, within the bound.
A program may use at most 128 MiB of HBM per device.

```python
import math
import jax
import jax.numpy as jnp
import numpy as np
from jax import lax

D = 4096
HQ = 4
HD = 128
FF = 1024
TOK_DEV = 512
HALO = 2048
TOKENS = 65536
DOCS = 64
N_DP = 32
N_FSDP = 4


def shared_query(key):
    base = jax.random.normal(jax.random.fold_in(key, 11), (D, HQ * HD), jnp.float32)
    return jnp.clip(base, -6.0, 6.0) / math.sqrt(D)


def draw_w_query(key, part):
    return shared_query(key).astype(jnp.bfloat16)


def draw_w_key_value(key, part):
    fresh = jax.random.normal(jax.random.fold_in(key, 23), (D, 2 * HD), jnp.float32)
    fresh = jnp.clip(fresh, -6.0, 6.0) / math.sqrt(D)
    return fresh.astype(jnp.bfloat16)


def block_levels(stream_key, extent, split, smallest, high):
    def one(dim, parts):
        steps = jax.random.uniform(jax.random.fold_in(jax.random.fold_in(stream_key, 6), dim), (parts,), jnp.float32, smallest / len(split), high / len(split))
        return jnp.repeat(jnp.exp(steps), extent[dim] // parts).reshape((-1,) + (1,) * (len(extent) - dim - 1))

    level = one(*split[0])
    for cut in split[1:]:
        level = level * one(*cut)
    return level


def split_up(count, total, most, slope):
    weights = [(1 << 20) // math.isqrt(grade ** slope) + 1 for grade in range(2, count + 1)]
    rest, holding = total - most - (count - 1), [1] * (count - 1)
    while rest > 0:
        movable = [i for i in range(count - 1) if holding[i] < most]
        whole, remaining = sum([weights[i] for i in movable]), rest
        for i in movable:
            addition = min(most - holding[i], max(1, remaining * weights[i] // whole), rest)
            holding[i] = holding[i] + addition
            rest = rest - addition
    return np.array([most] + holding)


def ragged_sizes(own_key, number_of, total, most, skew):
    if number_of == 2:
        one = jax.random.randint(own_key, (), max(1, total - most), min(most, total - 1) + 1)
        return jnp.stack([one, total - one])
    sizes = jnp.asarray(split_up(number_of, total, most, skew), jnp.int32)
    pairs = (number_of - 1) // 2
    donor, receiver = sizes[1:1 + 2 * pairs:2], sizes[2:2 + 2 * pairs:2]
    margin = jnp.minimum(donor - 1, most - receiver)
    passed = jax.random.randint(jax.random.fold_in(own_key, 1), (pairs,), 0, 1 << 20) % (margin + 1)
    sizes = sizes.at[1:1 + 2 * pairs:2].set(donor - passed).at[2:2 + 2 * pairs:2].set(receiver + passed)
    return sizes[jax.random.permutation(jax.random.fold_in(own_key, 2), number_of)]


def noise(stream_key, extent, spread, limit, shards=(), kind=jnp.bfloat16):
    values = spread * jax.random.normal(stream_key, extent, jnp.float32)
    if shards:
        values = values * block_levels(stream_key, extent, shards, -0.22, 0.18)
    return jnp.clip(values, -limit, limit).astype(kind)


def setup_inputs(seed: int = 0) -> dict:
    splits = jax.random.split(jax.random.key(seed), 11)
    return {
        "tokens": noise(splits[0], (TOKENS, D), 0.05, 0.75, ((0, 128),)),
        "doc_ids": jnp.searchsorted(jnp.cumsum(ragged_sizes(splits[1], DOCS, TOKENS, HALO, 1)), jnp.arange(TOKENS), side="right").astype(jnp.int32),
        "attn_gain": jnp.clip(1.0 + 0.18 * jax.random.normal(splits[2], (D,), jnp.float32), 0.1, 1.9),
        "mlp_gain": jnp.clip(1.0 + 0.18 * jax.random.normal(splits[3], (D,), jnp.float32), 0.1, 1.9),
        "w_query": draw_w_query(jax.random.fold_in(splits[10], 71), 0),
        "w_key_value": draw_w_key_value(jax.random.fold_in(splits[10], 71), 0),
        "w_out": noise(splits[6], (HQ * HD, D), (HQ * HD) ** -0.5, 0.25, ((1, 128),)),
        "w_gate": noise(splits[7], (D, FF), D ** -0.5, 0.09375, ((0, 128),)),
        "w_up": noise(splits[8], (D, FF), D ** -0.5, 0.09375, ((0, 128),)),
        "w_down": noise(splits[9], (FF, D), FF ** -0.5, 0.1875, ((1, 128),)),
    }


EPS = 1e-05
THETA = 500000.0
NEGATIVE = -1e+30

def rms_scale(values, gain):
    wide = values.astype(jnp.float32)
    power = lax.optimization_barrier(jnp.mean(wide * wide, axis=-1, keepdims=True))
    return (wide * lax.rsqrt(power + EPS) * gain).astype(jnp.bfloat16)

def rotate(values, position):
    head = values.shape[-1]
    half = head // 2
    freqs = THETA ** (-2.0 * jnp.arange(half, dtype=jnp.float32) / head)
    angle = position.astype(jnp.float32)[:, None, None] * freqs[None, None, :]
    cosine = jnp.cos(angle)
    sine = jnp.sin(angle)
    first = values[..., :half]
    second = values[..., half:]
    return jnp.concatenate([first * cosine - second * sine, second * cosine + first * sine], axis=-1)

def widen(values):
    return lax.optimization_barrier(values).astype(jnp.float32)

def attend(query, keys, values, key_marks, marks, offset):
    scores = jnp.einsum('qhd,kd->hqk', widen(query), widen(keys)) / math.sqrt(query.shape[-1])
    key_index = jnp.arange(keys.shape[0], dtype=jnp.int32)
    query_index = jnp.arange(query.shape[0], dtype=jnp.int32) + offset
    allowed = (key_marks[None, :] == marks[:, None]) & (key_index[None, :] <= query_index[:, None])
    scores = jnp.where(allowed[None, :, :], scores, NEGATIVE)
    peak = lax.optimization_barrier(jnp.max(scores, axis=2, keepdims=True))
    weights = jnp.exp(scores - peak)
    totals = lax.optimization_barrier(jnp.sum(weights, axis=2))
    mixed = jnp.einsum('hqk,kd->qhd', widen(weights.astype(jnp.bfloat16)), widen(values))
    return mixed / jnp.transpose(totals)[:, :, None]

def reference(tokens, doc_ids, attn_gain, mlp_gain, w_query, w_key_value, w_out, w_gate, w_up, w_down):
    total_rows = tokens.shape[0]
    normed = rms_scale(tokens, attn_gain)
    query_raw = jnp.dot(normed, w_query, preferred_element_type=jnp.float32)
    pair_raw = jnp.dot(normed, w_key_value, preferred_element_type=jnp.float32)
    position = jnp.arange(total_rows, dtype=jnp.int32)
    query = rotate(query_raw.reshape(total_rows, HQ, HD), position).astype(jnp.bfloat16)
    keys = rotate(pair_raw[:, None, :HD], position)[:, 0, :].astype(jnp.bfloat16)
    values = pair_raw[:, HD:].astype(jnp.bfloat16)
    marks = doc_ids + 1
    key_padded = jnp.concatenate([jnp.zeros((HALO, HD), jnp.bfloat16), keys], axis=0)
    value_padded = jnp.concatenate([jnp.zeros((HALO, HD), jnp.bfloat16), values], axis=0)
    mark_padded = jnp.concatenate([jnp.zeros((HALO,), jnp.int32), marks], axis=0)

    def one_rank(rank):
        start = (rank * TOK_DEV).astype(jnp.int32)
        rank_query = lax.dynamic_slice_in_dim(query, start, TOK_DEV, 0)
        rank_marks = lax.dynamic_slice_in_dim(marks, start, TOK_DEV, 0)
        rank_keys = lax.dynamic_slice_in_dim(key_padded, start, HALO + TOK_DEV, 0)
        rank_values = lax.dynamic_slice_in_dim(value_padded, start, HALO + TOK_DEV, 0)
        key_marks = lax.dynamic_slice_in_dim(mark_padded, start, HALO + TOK_DEV, 0)
        mixed = attend(rank_query, rank_keys, rank_values, key_marks, rank_marks, HALO)
        return mixed.reshape(TOK_DEV, HQ * HD).astype(jnp.bfloat16)
    attended = lax.map(one_rank, jnp.arange(N_DP * N_FSDP, dtype=jnp.int32)).reshape(total_rows, HQ * HD)
    projected = jnp.dot(attended, w_out, preferred_element_type=jnp.float32)
    resid = (tokens.astype(jnp.float32) + projected).astype(jnp.bfloat16)
    resid = lax.optimization_barrier(resid)
    normed_mlp = rms_scale(resid, mlp_gain)
    gate = jnp.dot(normed_mlp, w_gate, preferred_element_type=jnp.float32)
    up_value = jnp.dot(normed_mlp, w_up, preferred_element_type=jnp.float32)
    hidden = (jax.nn.silu(gate) * up_value).astype(jnp.bfloat16)
    down = jnp.dot(hidden, w_down, preferred_element_type=jnp.float32)
    return (resid.astype(jnp.float32) + down).astype(jnp.bfloat16)
```

```python
import functools
import math

import jax
import jax.numpy as jnp
from jax import lax
from jax.experimental import pallas as pl
from jax.experimental.pallas import tpu as pltpu
from jax.sharding import PartitionSpec as P

MESH = pl.DeviceIdType.MESH
EPS = 1e-05
THETA = 500000.0
NEGATIVE = -1e30
SIDE = 4
SPAN = 4
GROUPS = (
    ((0, 256), (256, 256), (512, 256)),
    ((768, 128), (896, 128), (1024, 256)),
    ((1280, 640), (1920, 640), (2560, 768)),
    ((3328, 384), (3712, 384), (4096, 256)),
)
ORDERS = (("x", "y", "z"), ("y", "z", "x"), ("z", "x", "y"))
OUT_AT, GATE_AT, UP_AT, DOWN_AT, WIDTH = 768, 1280, 2304, 3328, 4352
A_AT, B_AT, C_AT, PARTNER_AT, SLOTS = 0, 3, 9, 15, 19


def kernel(
    tok, gain_attn, gain_mlp, cosine, sine, doc_row, doc_col, wq, wkv, wo, wg, wu, wd,
    out,
    w, res, nrm, qry, keys, vals, marks, att, hid,
    send, recv, halo_send, halo_recv, local_sem, tok_sem, out_sem,
):
    rows, width = res.shape
    head = qry.shape[2]
    shard = wq.shape[0]
    half = shard // 2
    dp = lax.axis_index("dp")
    x = lax.axis_index("fsdp")
    y = dp // (2 * SIDE)
    z = (dp // 2) % SIDE
    c = dp % 2
    pos = {"x": x, "y": y, "z": z}
    rank = dp * SIDE + x
    ranks = 32 * SIDE

    def device(at, core):
        return ((at["y"] * SIDE + at["z"]) * 2 + core, at["x"])

    def shift(dim, by):
        return {**pos, dim: (pos[dim] + by) % SIDE}

    def peer(dim, by):
        return device(shift(dim, by), c)

    def at_rank(by):
        other = (rank + by + ranks) % ranks
        return (other // SIDE, other % SIDE)

    local = []
    for k, (src, at) in enumerate(
        ((wq, 0), (wkv, 512), (wo, OUT_AT), (wg, GATE_AT), (wu, UP_AT), (wd, DOWN_AT))
    ):
        local.append(
            pltpu.make_async_copy(
                src, w.at[y, z, c, x, :, pl.ds(at, src.shape[1])], local_sem.at[k]
            )
        )
    for copy in local:
        copy.start()
    chunk = rows // 4
    tok_copies = [
        pltpu.make_async_copy(
            tok.at[pl.ds(k * chunk, chunk)], res.at[pl.ds(k * chunk, chunk)], tok_sem.at[k]
        )
        for k in range(4)
    ]
    for copy in tok_copies:
        copy.start()

    barrier = pltpu.get_barrier_semaphore()
    friends = [peer(dim, by) for dim in ("x", "y", "z") for by in (1, 2, 3)]
    friends.append(device(pos, 1 - c))
    friends += [at_rank(by) for by in range(-SPAN, SPAN + 1) if by != 0]
    for friend in friends:
        pl.semaphore_signal(barrier, inc=1, device_id=friend, device_id_type=MESH)
    pl.semaphore_wait(barrier, len(friends))

    sends = []

    def block(core, sel, part, r0, nr):
        at, n = part
        return w.at[
            sel["y"], sel["z"], core, sel["x"], pl.ds(r0, nr), pl.ds(at, n)
        ]

    def remote(ref, row, slot, to):
        return pltpu.make_async_remote_copy(
            src_ref=ref, dst_ref=ref, send_sem=send.at[row, slot], recv_sem=recv.at[row, slot],
            device_id=to, device_id_type=MESH,
        )

    def push(ref, row, slot, to):
        copy = remote(ref, row, slot, to)
        copy.start()
        sends.append(copy)

    ALL = slice(None)

    def each(g):
        for p in range(3):
            yield g * 3 + p, GROUPS[g][p], ORDERS[p]

    def spread(row, part, dim, base, done):
        sel = {**pos, **{d: ALL for d in done}}
        push(block(c, sel, part, 0, half), row, base + 0, peer(dim, 1))
        push(block(c, sel, part, half, half), row, base + 3, peer(dim, -1))
        push(block(c, sel, part, half, half), row, base + 1, peer(dim, 1))
        push(block(c, sel, part, 0, half), row, base + 2, peer(dim, -1))

    def relay(row, part, dim, base, done):
        back = {**shift(dim, -1), **{d: ALL for d in done}}
        ahead = {**shift(dim, 1), **{d: ALL for d in done}}
        ref = block(c, back, part, 0, half)
        remote(ref, row, base + 0, peer(dim, 1)).wait_recv()
        push(ref, row, base + 4, peer(dim, 1))
        ref = block(c, ahead, part, half, half)
        remote(ref, row, base + 3, peer(dim, 1)).wait_recv()
        push(ref, row, base + 5, peer(dim, -1))

    def near(row, part, dim, base, done):
        back = {**shift(dim, -1), **{d: ALL for d in done}}
        ahead = {**shift(dim, 1), **{d: ALL for d in done}}
        remote(block(c, back, part, half, half), row, base + 1, peer(dim, 1)).wait_recv()
        remote(block(c, ahead, part, 0, half), row, base + 2, peer(dim, 1)).wait_recv()

    def far(row, part, dim, base, done):
        across = {**shift(dim, 2), **{d: ALL for d in done}}
        remote(block(c, across, part, 0, half), row, base + 4, peer(dim, 1)).wait_recv()
        remote(block(c, across, part, half, half), row, base + 5, peer(dim, 1)).wait_recv()

    def partner_ref(core, part, order, by):
        sel = {order[0]: ALL, order[1]: ALL, order[2]: (pos[order[2]] + by) % SIDE}
        return block(core, sel, part, 0, shard)

    def to_partner(row, part, order, by):
        push(partner_ref(c, part, order, by), row, PARTNER_AT + by, device(pos, 1 - c))

    def first(g):
        for row, part, order in each(g):
            for by in (1, 3, 2):
                push(block(c, pos, part, 0, shard), row, A_AT + by - 1, peer(order[0], by))

    def second(g):
        for row, part, order in each(g):
            for by in (1, 3, 2):
                ref = block(c, shift(order[0], -by), part, 0, shard)
                remote(ref, row, A_AT + by - 1, peer(order[0], by)).wait_recv()
            spread(row, part, order[1], B_AT, order[:1])

    def second_relay(g):
        for row, part, order in each(g):
            relay(row, part, order[1], B_AT, order[:1])

    def third(g):
        for row, part, order in each(g):
            near(row, part, order[1], B_AT, order[:1])
            far(row, part, order[1], B_AT, order[:1])
            spread(row, part, order[2], C_AT, order[:2])
        for row, part, order in each(g):
            to_partner(row, part, order, 0)

    def third_relay(g):
        for row, part, order in each(g):
            relay(row, part, order[2], C_AT, order[:2])

    def third_near(g):
        for row, part, order in each(g):
            near(row, part, order[2], C_AT, order[:2])
            to_partner(row, part, order, 1)
            to_partner(row, part, order, 3)

    def third_far(g):
        for row, part, order in each(g):
            far(row, part, order[2], C_AT, order[:2])
            to_partner(row, part, order, 2)

    def finish(g):
        for row, part, order in each(g):
            for by in range(SIDE):
                ref = partner_ref(1 - c, part, order, by)
                remote(ref, row, PARTNER_AT + by, device(pos, 1 - c)).wait_recv()

    def halo(src, dst, slot, by):
        return pltpu.make_async_remote_copy(
            src_ref=src, dst_ref=dst, send_sem=halo_send.at[slot, by], recv_sem=halo_recv.at[slot, by],
            device_id=at_rank(by), device_id_type=MESH,
        )

    def norm(gain, r0, n):
        def step(k, carry):
            at = pl.ds(pl.multiple_of(r0 + k * 16, 16), 16)
            wide = res[at, :].astype(jnp.float32)
            power = jnp.mean(wide * wide, axis=-1, keepdims=True)
            nrm[at, :] = (wide * lax.rsqrt(power + EPS) * gain[...]).astype(jnp.bfloat16)
            return carry

        lax.fori_loop(0, n // 16, step, 0)

    def columns(at, n):
        return w[:, :, :, :, :, pl.ds(at, n)].reshape(width, n)

    def rotated(u):
        return u * cosine[...] + pltpu.roll(u, head // 2, 1) * sine[...]

    for copy in local:
        copy.wait()
    for g in range(4):
        first(g)
    for by in range(1, SPAN + 1):
        copy = halo(doc_row, marks.at[SPAN - by], 2, by)
        copy.start()
        sends.append(copy)
    marks[SPAN] = doc_row[...]

    tok_copies[0].wait()
    norm(gain_attn, 0, chunk)
    second(0)
    tok_copies[1].wait()
    norm(gain_attn, chunk, chunk)
    second_relay(0)
    tok_copies[2].wait()
    norm(gain_attn, 2 * chunk, chunk)
    third(0)
    second(1)
    tok_copies[3].wait()
    norm(gain_attn, 3 * chunk, chunk)
    third_relay(0)
    second_relay(1)
    third_near(0)
    third(1)
    third_far(0)
    finish(0)

    pair = jnp.dot(nrm[...], columns(512, 256), preferred_element_type=jnp.float32)
    keys[SPAN] = jnp.transpose(rotated(pair[:, :head])).astype(jnp.bfloat16)
    vals[SPAN] = pair[:, head:].astype(jnp.bfloat16)
    third_relay(1)
    second(2)
    for p in range(2):
        raw = jnp.dot(nrm[...], columns(256 * p, 256), preferred_element_type=jnp.float32)
        if p == 0:
            for by in range(1, SPAN + 1):
                for slot, buf in ((0, keys), (1, vals)):
                    copy = halo(buf.at[SPAN], buf.at[SPAN - by], slot, by)
                    copy.start()
                    sends.append(copy)
            second(3)
        for k in range(2):
            qry[2 * p + k] = rotated(raw[:, k * head : (k + 1) * head]).astype(jnp.bfloat16)
        if p == 0:
            third_near(1)
            second_relay(2)
    third(2)
    third_far(1)
    second_relay(3)

    for by in range(1, SPAN + 1):
        halo(doc_row, marks.at[SPAN - by], 2, by).wait_recv()
        for slot, buf in ((0, keys), (1, vals)):
            halo(buf.at[SPAN], buf.at[SPAN - by], slot, by).wait_recv()

    tall = rows // 2
    scale = math.log2(math.e) / math.sqrt(head)

    def attend(part, h):
        spans = (
            [(j, 0, rows) for j in range(SPAN)] + [(SPAN, 0, tall)]
            if part == 0
            else [(0, tall, tall)]
            + [(j, 0, rows) for j in range(1, SPAN)]
            + [(SPAN, 0, tall), (SPAN, tall, tall)]
        )
        q = qry[h, part * tall : (part + 1) * tall, :]
        mine = doc_col[part * tall : (part + 1) * tall, :]
        scores = []
        for k, (j, at, n) in enumerate(spans):
            s = jnp.dot(q, keys[j, :, at : at + n], preferred_element_type=jnp.float32)
            same = marks[j, 0:1, at : at + n] == mine
            if k == len(spans) - 1:
                same = same & (
                    lax.broadcasted_iota(jnp.int32, (tall, n), 1)
                    <= lax.broadcasted_iota(jnp.int32, (tall, n), 0)
                )
            scores.append(jnp.where(same, s, NEGATIVE))
        peak = functools.reduce(
            jnp.maximum, [jnp.max(s, axis=1, keepdims=True) for s in scores]
        )
        total = jnp.zeros((tall, 1), jnp.float32)
        mixed = jnp.zeros((tall, head), jnp.float32)
        for (j, at, n), s in zip(spans, scores):
            e = jnp.exp2((s - peak) * scale)
            total = total + jnp.sum(e, axis=1, keepdims=True)
            mixed = mixed + jnp.dot(
                e.astype(jnp.bfloat16), vals[j, at : at + n, :], preferred_element_type=jnp.float32
            )
        att[part * tall : (part + 1) * tall, pl.ds(pl.multiple_of(h * head, head), head)] = (
            mixed / total
        ).astype(jnp.bfloat16)

    def attend_heads(part, lo, hi):
        def step(h, carry):
            attend(part, h)
            return carry

        lax.fori_loop(lo, hi, step, 0)

    attend_heads(0, 0, 2)
    finish(1)
    third_relay(2)
    third(3)
    attend_heads(0, 2, 4)
    third_near(2)
    attend_heads(1, 0, 2)
    attend_heads(1, 2, 4)

    def wide_step(lhs, at, n, after):
        per = 2 * 2 * SIDE * shard

        def step(k, carry):
            for zz in range(2):
                rhs = w[k, 2 * zz : 2 * zz + 2, :, :, :, at : at + n].reshape(per, n)
                got = lax.dot_general(
                    lhs[...], rhs, (((1,), (1,)), ((), ())), preferred_element_type=jnp.float32
                )
                here = pl.ds(pl.multiple_of((k * 2 + zz) * per, per), per)
                res[:, here] = (res[:, here].astype(jnp.float32) + got).astype(jnp.bfloat16)
            after(k)
            return carry

        lax.fori_loop(0, SIDE, step, 0)

    wide_step(att, OUT_AT, 512, lambda k: None)
    third_relay(3)
    norm(gain_mlp, 0, rows // 2)
    third_far(2)
    norm(gain_mlp, rows // 2, rows // 2)
    finish(2)

    def gated(lo, hi):
        def step(j, carry):
            at = pl.multiple_of(j * 256, 256)
            gate = jnp.dot(nrm[...], columns(GATE_AT + at, 256), preferred_element_type=jnp.float32)
            up = jnp.dot(nrm[...], columns(UP_AT + at, 256), preferred_element_type=jnp.float32)
            hid[:, pl.ds(at, 256)] = (gate / (1.0 + jnp.exp(-gate)) * up).astype(jnp.bfloat16)
            return carry

        lax.fori_loop(lo, hi, step, 0)

    gated(0, 2)
    third_near(3)
    gated(2, 4)
    third_far(3)
    finish(3)

    slab = width // SIDE

    def put(k):
        here = pl.ds(pl.multiple_of(k * slab, slab), slab)
        return pltpu.make_async_copy(res.at[:, here], out.at[:, here], out_sem.at[k])

    wide_step(hid, DOWN_AT, 1024, lambda k: put(k).start())
    for k in range(SIDE):
        put(k).wait()
    for copy in sends:
        copy.wait_send()


def per_device(
    tokens, doc_ids, attn_gain, mlp_gain, w_query, w_key_value, w_out, w_gate, w_up, w_down
):
    rows, width = tokens.shape
    head = w_key_value.shape[1] // 2
    heads = w_query.shape[1] // head
    shard = w_query.shape[0]
    rank = lax.axis_index(("dp", "fsdp"))
    freqs = THETA ** (-2.0 * jnp.arange(head // 2, dtype=jnp.float32) / head)
    position = rank * rows + jnp.arange(rows, dtype=jnp.int32)
    angle = position.astype(jnp.float32)[:, None] * freqs[None, :]
    cosine = jnp.cos(angle)
    sine = jnp.sin(angle)
    cosine = jnp.concatenate([cosine, cosine], axis=1)
    sine = jnp.concatenate([-sine, sine], axis=1)
    doc_row = jnp.broadcast_to(doc_ids[None, :], (8, rows))
    vmem = pl.BlockSpec(memory_space=pltpu.VMEM)
    anywhere = pl.BlockSpec(memory_space=pl.ANY)
    bf16 = jnp.bfloat16
    return pl.pallas_call(
        kernel,
        out_shape=jax.ShapeDtypeStruct((rows, width), bf16),
        in_specs=[anywhere] + [vmem] * 6 + [anywhere] * 6,
        out_specs=anywhere,
        scratch_shapes=[
            pltpu.VMEM((SIDE, SIDE, 2, SIDE, shard, WIDTH), bf16),
            pltpu.VMEM((rows, width), bf16),
            pltpu.VMEM((rows, width), bf16),
            pltpu.VMEM((heads, rows, head), bf16),
            pltpu.VMEM((SPAN + 1, head, rows), bf16),
            pltpu.VMEM((SPAN + 1, rows, head), bf16),
            pltpu.VMEM((SPAN + 1, 8, rows), jnp.int32),
            pltpu.VMEM((rows, heads * head), bf16),
            pltpu.VMEM((rows, w_gate.shape[1]), bf16),
            pltpu.SemaphoreType.DMA((12, SLOTS)),
            pltpu.SemaphoreType.DMA((12, SLOTS)),
            pltpu.SemaphoreType.DMA((3, SPAN + 1)),
            pltpu.SemaphoreType.DMA((3, SPAN + 1)),
            pltpu.SemaphoreType.DMA((6,)),
            pltpu.SemaphoreType.DMA((4,)),
            pltpu.SemaphoreType.DMA((SIDE,)),
        ],
        compiler_params=pltpu.CompilerParams(
            collective_id=0, has_side_effects=True, vmem_limit_bytes=67043328
        ),
    )(
        tokens,
        attn_gain[None, :],
        mlp_gain[None, :],
        cosine,
        sine,
        doc_row,
        doc_ids[:, None],
        w_query,
        w_key_value,
        w_out.T,
        w_gate,
        w_up,
        w_down.T,
    )


def solution(mesh):
    every = ("dp", "fsdp")
    in_specs = (
        P(every, None), P(every), P(), P(), P(every, None), P(every, None),
        P(None, every), P(every, None), P(every, None), P(None, every),
    )
    return jax.shard_map(
        per_device, mesh=mesh, in_specs=in_specs, out_specs=P(every, None), check_vma=False
    )
```

```python
import functools
import math

import jax
import jax.numpy as jnp
import numpy as np
from jax import lax
from jax.experimental import pallas as pl
from jax.experimental.pallas import tpu as pltpu
from jax.sharding import PartitionSpec as P

MESH = pl.DeviceIdType.MESH
EPS = 1e-05
THETA = 500000.0
NEGATIVE = -1e30
SIDE = 4
SPAN = 4
GROUPS = (
    ((0, 128, 0), (128, 128, 2)),
    ((256, 384, 0), (640, 256, 1), (896, 512, 2)),
    ((1408, 640, 0), (2048, 640, 1), (2688, 640, 2)),
    ((3328, 256, 0), (3584, 384, 1), (3968, 384, 2)),
)
ORDERS = (("x", "y", "z"), ("y", "z", "x"), ("z", "x", "y"))
PAIR_AT, QUERY_AT, OUT_AT, GATE_AT, UP_AT, DOWN_AT, WIDTH = 0, 256, 768, 1280, 2304, 3328, 4352
ARRIVALS = 104


def kernel(
    tok, gain_attn, gain_mlp, freqs, docs, wq, wkv, wo, wg, wu, wd,
    res,
    w, nrm, qry, keys, vals, marks, mine, cosine, sine, power, att, hid,
    send, recv, local_sem, tok_sem,
):
    rows, width = res.shape
    head = qry.shape[2]
    shard = wq.shape[0]
    half = shard // 2
    dp = lax.axis_index("dp")
    x = lax.axis_index("fsdp")
    y = dp // (2 * SIDE)
    z = (dp // 2) % SIDE
    c = dp % 2
    pos = {"x": x, "y": y, "z": z}
    rank = dp * SIDE + x
    ranks = 32 * SIDE

    def device(at, core):
        return ((at["y"] * SIDE + at["z"]) * 2 + core, at["x"])

    def shift(dim, by):
        return {**pos, dim: (pos[dim] + by) % SIDE}

    def peer(dim, by):
        return device(shift(dim, by), c)

    def at_rank(by):
        other = (rank + by + ranks) % ranks
        return (other // SIDE, other % SIDE)

    local = []
    for k, (src, at) in enumerate(
        ((wkv, PAIR_AT), (wq, QUERY_AT), (wo, OUT_AT), (wg, GATE_AT), (wu, UP_AT), (wd, DOWN_AT))
    ):
        local.append(
            pltpu.make_async_copy(
                src, w.at[y, z, c, x, :, pl.ds(at, src.shape[1])], local_sem.at[0]
            )
        )
    for copy in local:
        copy.start()
    chunk = rows // 4
    tok_copies = [
        pltpu.make_async_copy(
            tok.at[pl.ds(k * chunk, chunk)], res.at[pl.ds(k * chunk, chunk)], tok_sem.at[k]
        )
        for k in range(4)
    ]
    for copy in tok_copies:
        copy.start()

    barrier = pltpu.get_barrier_semaphore()
    friends = [peer(dim, by) for dim in ("x", "y", "z") for by in (1, 2, 3)]
    friends.append(device(pos, 1 - c))
    friends += [at_rank(by) for by in range(-SPAN, SPAN + 1) if by != 0]
    for friend in friends:
        pl.semaphore_signal(barrier, inc=1, device_id=friend, device_id_type=MESH)
    pl.semaphore_wait(barrier, len(friends))

    arrivals = {}

    def arrival(*key):
        return recv.at[arrivals.setdefault(key, len(arrivals))]

    def block(core, sel, part, r0, nr):
        at, n = part
        return w.at[
            sel["y"], sel["z"], core, sel["x"], pl.ds(r0, nr), pl.ds(at, n)
        ]

    def remote(ref, key, to, sent=0):
        return pltpu.make_async_remote_copy(
            src_ref=ref, dst_ref=ref, send_sem=send.at[sent], recv_sem=arrival(*key),
            device_id=to, device_id_type=MESH,
        )

    def push(ref, key, to, sent):
        remote(ref, key, to, sent).start()

    ALL = slice(None)

    def each(g):
        for p, (at, n, o) in enumerate(GROUPS[g]):
            yield g * 3 + p, (at, n), ORDERS[o]

    def keys_of(row, k):
        at = (row, k)
        near_key, far_key = ((*at, 2), (*at, 2)) if k < 2 else ((*at, 2), (*at, 3))
        return (*at, 0), (*at, 1), near_key, far_key

    def spread(row, part, order, k):
        dim = order[k]
        up, down, close, _ = keys_of(row, k)
        sel = {**pos, **{d: ALL for d in order[:k]}}
        push(block(c, sel, part, 0, half), up, peer(dim, 1), k)
        push(block(c, sel, part, half, half), down, peer(dim, -1), k)
        push(block(c, sel, part, half, half), close, peer(dim, 1), k)
        push(block(c, sel, part, 0, half), close, peer(dim, -1), k)

    def relay(row, part, order, k):
        dim = order[k]
        up, down, _, distant = keys_of(row, k)
        back = {**shift(dim, -1), **{d: ALL for d in order[:k]}}
        ahead = {**shift(dim, 1), **{d: ALL for d in order[:k]}}
        ref = block(c, back, part, 0, half)
        remote(ref, up, peer(dim, 1)).wait_recv()
        push(ref, distant, peer(dim, 1), k)
        ref = block(c, ahead, part, half, half)
        remote(ref, down, peer(dim, 1)).wait_recv()
        push(ref, distant, peer(dim, -1), k)

    def whole(row, part, order, k, blocks, key):
        dim = order[k]
        sel = {**pos, dim: pl.ds(0, blocks), **{d: ALL for d in order[:k]}}
        remote(block(c, sel, part, 0, shard), key, peer(dim, 1)).wait_recv()

    def near(row, part, order, k):
        whole(row, part, order, k, 1, keys_of(row, k)[2])

    def far(row, part, order, k):
        whole(row, part, order, k, 1, keys_of(row, k)[3])

    def both(row, part, order, k):
        whole(row, part, order, k, 2, keys_of(row, k)[2])

    def ring(k, what, g, only=None):
        for row, part, order in each(g):
            if only is None or order[2] in only:
                what(row, part, order, k)

    def direct(k, g):
        for row, part, order in each(g):
            sel = {**pos, **{d: ALL for d in order[:k]}}
            for by in (1, 3, 2):
                push(block(c, sel, part, 0, shard), ("direct", k, g), peer(order[k], by), k)

    def span(g):
        lo, hi = GROUPS[g][0], GROUPS[g][-1]
        return pl.ds(lo[0], hi[0] + hi[1] - lo[0])

    def direct_wait(k, g):
        three = pl.ds(0, 3)
        ref = w.at[0, three, 0, ALL, ALL, span(g)] if k else w.at[0, 0, 0, three, ALL, span(g)]
        remote(ref, ("direct", k, g), device(pos, 1 - c)).wait_recv()

    def partner_ref(core, part, order, by):
        sel = {order[0]: ALL, order[1]: ALL, order[2]: (pos[order[2]] + by) % SIDE}
        return block(core, sel, part, 0, shard)

    def share(g, *which):
        for row, part, order in each(g):
            for by in which:
                push(partner_ref(c, part, order, by), ("share", g), device(pos, 1 - c), 3)

    def share_wait(g):
        ref = w.at[ALL, ALL, 1 - c, ALL, ALL, span(g)]
        remote(ref, ("share", g), device(pos, 1 - c)).wait_recv()

    def halo(src, dst, slot, by, to):
        key = ("halo", slot, by) if (slot, by) in ((0, 1), (1, 3)) else ("halo", slot)
        return pltpu.make_async_remote_copy(
            src_ref=src, dst_ref=dst, send_sem=send.at[4 + slot], recv_sem=arrival(*key),
            device_id=at_rank(to), device_id_type=MESH,
        )

    def norm(gain, r0, n):
        def step(k, carry):
            at = pl.ds(pl.multiple_of(r0 + k * 16, 16), 16)
            wide = res[at, :].astype(jnp.float32)
            power = jnp.mean(wide * wide, axis=-1, keepdims=True)
            nrm[at, :] = (wide * lax.rsqrt(power + EPS) * gain[...]).astype(jnp.bfloat16)
            return carry

        lax.fori_loop(0, n // 16, step, 0)

    def columns(at, n):
        return w[:, :, :, :, :, pl.ds(at, n)].reshape(width, n)

    def rotated(u):
        return u * cosine[...] + pltpu.roll(u, head // 2, 1) * sine[...]

    scope = jax.named_scope

    def pass_on(src, dst, slot, by, to):
        halo(src, dst, slot, by, to).start()

    def halo_wait(slot, by):
        buf = (keys, vals)[slot]
        halo(buf.at[SPAN], buf.at[SPAN - by], slot, by, by).wait_recv()

    def halo_rest(slot, n):
        ref = (keys, vals, marks)[slot].at[pl.ds(0, n)]
        halo(ref, ref, slot, 4, 4).wait_recv()

    marks[SPAN] = jnp.broadcast_to(docs[...], (8, rows))
    with scope("local"):
        own = w.at[y, z, c, x]
        pltpu.make_async_copy(own, own, local_sem.at[0]).wait()
    for g in (0, 1):
        direct(0, g)
    for g in (2, 3):
        ring(0, spread, g)
    turned = docs[...].astype(jnp.float32)
    mine[...] = jnp.transpose(jnp.broadcast_to(turned, (head, rows))).astype(jnp.int32)
    with scope("norm0"):
        tok_copies[0].wait()
        norm(gain_attn, 0, chunk)
    with scope("B0"):
        direct_wait(0, 0)
        direct(1, 0)
    with scope("B1"):
        direct_wait(0, 1)
        ring(1, spread, 1)
    with scope("Ar"):
        for g in (2, 3):
            ring(0, relay, g)
    for by in range(1, SPAN + 1):
        pass_on(marks.at[SPAN], marks.at[SPAN - by], 2, by, by)
    with scope("norm1"):
        tok_copies[1].wait()
        norm(gain_attn, chunk, chunk)
    with scope("C0"):
        direct_wait(1, 0)
        ring(2, spread, 0)
        share(0, 0)
    with scope("B2"):
        ring(0, both, 2)
        ring(1, spread, 2)
    with scope("norm2"):
        tok_copies[2].wait()
        norm(gain_attn, 2 * chunk, chunk)
    with scope("Br1"):
        ring(1, relay, 1)
    with scope("B3"):
        ring(0, both, 3)
        ring(1, spread, 3)
    with scope("Cr0"):
        ring(2, relay, 0)
    with scope("angles"):
        place = rank * rows + lax.broadcasted_iota(jnp.int32, (rows, head), 0)
        angle = place.astype(jnp.float32) * freqs[...]
        cosine[...] = jnp.cos(angle)
        turn = jnp.sin(angle)
        early = lax.broadcasted_iota(jnp.int32, (rows, head), 1) < head // 2
        sine[...] = jnp.where(early, -turn, turn)
    with scope("near0"):
        ring(2, near, 0)
        share(0, 1, 3)
    with scope("Br2"):
        ring(1, relay, 2)
    with scope("C1"):
        ring(1, both, 1)
        ring(2, spread, 1)
    with scope("norm3"):
        tok_copies[3].wait()
        norm(gain_attn, 3 * chunk, chunk)
    with scope("far0"):
        ring(2, far, 0)
        share(0, 2)
    with scope("Br3"):
        ring(1, relay, 3)
    with scope("F0"):
        share_wait(0)

    with scope("pair"):
        pair = jnp.dot(nrm[...], columns(PAIR_AT, 256), preferred_element_type=jnp.float32)
        keys[SPAN] = jnp.transpose(rotated(pair[:, :head])).astype(jnp.bfloat16)
        vals[SPAN] = pair[:, head:].astype(jnp.bfloat16)
    pass_on(keys.at[SPAN], keys.at[SPAN - 1], 0, 1, 1)
    pass_on(vals.at[SPAN], vals.at[SPAN - 3], 1, 3, 3)
    pass_on(vals.at[SPAN], vals.at[SPAN - 1], 1, 1, 1)
    pass_on(keys.at[SPAN], keys.at[SPAN - 3], 0, 3, 3)
    pass_on(keys.at[SPAN], keys.at[SPAN - 4], 0, 4, 4)
    pass_on(vals.at[SPAN], vals.at[SPAN - 4], 1, 4, 4)
    with scope("Cr1zx"):
        share(1, 0)
        ring(2, relay, 1, "zx")
    with scope("Cr1y"):
        ring(2, relay, 1, "y")
    with scope("C2yz"):
        ring(1, both, 2)
        ring(2, spread, 2, "yz")
    with scope("forward"):
        halo_wait(0, 1)
        pass_on(keys.at[SPAN - 1], keys.at[SPAN - 2], 0, 2, 1)
        halo_wait(1, 3)
        pass_on(vals.at[SPAN - 3], vals.at[SPAN - 2], 1, 2, -1)
    with scope("C2x"):
        ring(2, spread, 2, "x")
    with scope("near1"):
        ring(2, near, 1)
        share(1, 1, 3)
    with scope("far1"):
        ring(2, far, 1)
        share(1, 2)
    with scope("F1"):
        share_wait(1)
        share(2, 0)
    with scope("query"):
        for p in range(2):
            raw = jnp.dot(nrm[...], columns(QUERY_AT + 256 * p, 256), preferred_element_type=jnp.float32)
            for k in range(2):
                qry[2 * p + k] = rotated(raw[:, k * head : (k + 1) * head]).astype(jnp.bfloat16)
    with scope("halo"):
        halo_rest(2, 4)
        halo_rest(0, 3)
        halo_rest(1, 3)

    tall = rows // 2
    scale = math.log2(math.e) / math.sqrt(head)

    def attend(part, h):
        spans = (
            [(j, 0, rows) for j in range(SPAN)] + [(SPAN, 0, tall)]
            if part == 0
            else [(0, tall, tall)]
            + [(j, 0, rows) for j in range(1, SPAN)]
            + [(SPAN, 0, tall), (SPAN, tall, tall)]
        )
        q = qry[h, part * tall : (part + 1) * tall, :]
        own = mine[part * tall : (part + 1) * tall, 0:1]
        scores = []
        for k, (j, at, n) in enumerate(spans):
            s = jnp.dot(q, keys[j, :, at : at + n], preferred_element_type=jnp.float32)
            same = marks[j, 0:1, at : at + n] == own
            if k == len(spans) - 1:
                same = same & (
                    lax.broadcasted_iota(jnp.int32, (tall, n), 1)
                    <= lax.broadcasted_iota(jnp.int32, (tall, n), 0)
                )
            scores.append(jnp.where(same, s, NEGATIVE))
        peak = functools.reduce(
            jnp.maximum, [jnp.max(s, axis=1, keepdims=True) for s in scores]
        )
        total = jnp.zeros((tall, 1), jnp.float32)
        mixed = jnp.zeros((tall, head), jnp.float32)
        for (j, at, n), s in zip(spans, scores):
            e = jnp.exp2((s - peak) * scale)
            total = total + jnp.sum(e, axis=1, keepdims=True)
            mixed = mixed + jnp.dot(
                e.astype(jnp.bfloat16), vals[j, at : at + n, :], preferred_element_type=jnp.float32
            )
        att[part * tall : (part + 1) * tall, pl.ds(pl.multiple_of(h * head, head), head)] = (
            mixed / total
        ).astype(jnp.bfloat16)

    def attend_heads(part, lo, hi):
        def step(h, carry):
            attend(part, h)
            return carry

        lax.fori_loop(lo, hi, step, 0)

    with scope("attend0"):
        attend_heads(0, 0, 2)
    with scope("Cr2"):
        ring(2, relay, 2)
    with scope("C3"):
        ring(1, both, 3)
        ring(2, spread, 3)
    with scope("attend1"):
        attend_heads(0, 2, 4)
    with scope("attend2"):
        attend_heads(1, 0, 2)
    with scope("near2"):
        ring(2, near, 2)
        share(2, 1, 3)
        share(3, 0)
    with scope("attend3"):
        attend_heads(1, 2, 4)

    def wide_step(lhs, at, n, after, squares=False):
        per = 2 * 2 * SIDE * shard

        def step(k, carry):
            for zz in range(2):
                rhs = w[k, 2 * zz : 2 * zz + 2, :, :, :, at : at + n].reshape(per, n)
                got = lax.dot_general(
                    lhs[...], rhs, (((1,), (1,)), ((), ())), preferred_element_type=jnp.float32
                )
                here = pl.ds(pl.multiple_of((k * 2 + zz) * per, per), per)
                new = (res[:, here].astype(jnp.float32) + got).astype(jnp.bfloat16)
                res[:, here] = new
                if squares:
                    wide = new.astype(jnp.float32)
                    wide = wide * wide
                    sums = [wide[:, i * head : (i + 1) * head] for i in range(per // head)]
                    power[...] += functools.reduce(jnp.add, sums)
            after(k)
            return carry

        lax.fori_loop(0, SIDE, step, 0)

    def scaled(gain):
        mean = jnp.sum(power[...], axis=-1, keepdims=True) / width
        power[...] = jnp.broadcast_to(lax.rsqrt(mean + EPS), (rows, head))

        def step(k, carry):
            at = pl.ds(pl.multiple_of(k * 32, 32), 32)
            inverse = power[at, :]
            for i in range(width // head):
                lanes = slice(i * head, (i + 1) * head)
                wide = res[at, lanes].astype(jnp.float32)
                nrm[at, lanes] = (wide * inverse * gain[:, lanes]).astype(jnp.bfloat16)
            return carry

        lax.fori_loop(0, rows // 32, step, 0)

    power[...] = jnp.zeros_like(power)
    with scope("project"):
        wide_step(att, OUT_AT, 512, lambda k: None, squares=True)
    with scope("far2"):
        ring(2, far, 2)
        share(2, 2)
    with scope("mlp_norm"):
        scaled(gain_mlp)
    with scope("Cr3"):
        ring(2, relay, 3)
    with scope("F2"):
        share_wait(2)

    def gated(lo, hi):
        def step(j, carry):
            at = pl.multiple_of(j * 256, 256)
            gate = jnp.dot(nrm[...], columns(GATE_AT + at, 256), preferred_element_type=jnp.float32)
            up = jnp.dot(nrm[...], columns(UP_AT + at, 256), preferred_element_type=jnp.float32)
            hid[:, pl.ds(at, 256)] = (gate / (1.0 + jnp.exp(-gate)) * up).astype(jnp.bfloat16)
            return carry

        lax.fori_loop(lo, hi, step, 0)

    with scope("gated0"):
        gated(0, 2)
    with scope("near3"):
        ring(2, near, 3)
        share(3, 1, 3)
    with scope("gated1"):
        gated(2, 4)
    with scope("F3"):
        ring(2, far, 3)
        share(3, 2)
        share_wait(3)

    with scope("down"):
        wide_step(hid, DOWN_AT, 1024, lambda k: None)
    assert len(arrivals) <= ARRIVALS
    with scope("sent"):
        three = pl.ds(0, 3)
        for k, ref in enumerate(
            (w.at[0, 0, 0, three], w.at[0, three, 0], w.at[three, ALL, 0], w.at[ALL, ALL, 0])
        ):
            remote(ref, ("share", 0), device(pos, 1 - c), k).wait_send()
        for slot, buf in enumerate((keys, vals, marks)):
            ref = buf.at[pl.ds(0, 4)]
            halo(ref, ref, slot, 4, 4).wait_send()


def per_device(
    tokens, doc_ids, attn_gain, mlp_gain, w_query, w_key_value, w_out, w_gate, w_up, w_down
):
    rows, width = tokens.shape
    head = w_key_value.shape[1] // 2
    heads = w_query.shape[1] // head
    shard = w_query.shape[0]
    freqs = THETA ** (-2.0 * np.arange(head // 2) / head)
    freqs = np.concatenate([freqs, freqs])[None, :].astype(np.float32)
    vmem = pl.BlockSpec(memory_space=pltpu.VMEM)
    anywhere = pl.BlockSpec(memory_space=pl.ANY)
    bf16 = jnp.bfloat16
    return pl.pallas_call(
        kernel,
        out_shape=pltpu.VMEM((rows, width), bf16),
        in_specs=[anywhere] + [vmem] * 4 + [anywhere] * 6,
        out_specs=vmem,
        scratch_shapes=[
            pltpu.VMEM((SIDE, SIDE, 2, SIDE, shard, WIDTH), bf16),
            pltpu.VMEM((rows, width), bf16),
            pltpu.VMEM((heads, rows, head), bf16),
            pltpu.VMEM((SPAN + 1, head, rows), bf16),
            pltpu.VMEM((SPAN + 1, rows, head), bf16),
            pltpu.VMEM((SPAN + 1, 8, rows), jnp.int32),
            pltpu.VMEM((rows, head), jnp.int32),
            pltpu.VMEM((rows, head), jnp.float32),
            pltpu.VMEM((rows, head), jnp.float32),
            pltpu.VMEM((rows, head), jnp.float32),
            pltpu.VMEM((rows, heads * head), bf16),
            pltpu.VMEM((rows, w_gate.shape[1]), bf16),
            pltpu.SemaphoreType.DMA((7,)),
            pltpu.SemaphoreType.DMA((ARRIVALS,)),
            pltpu.SemaphoreType.DMA((1,)),
            pltpu.SemaphoreType.DMA((4,)),
        ],
        compiler_params=pltpu.CompilerParams(
            collective_id=0, has_side_effects=True, vmem_limit_bytes=58 * 1024 * 1024
        ),
    )(
        tokens,
        attn_gain[None, :],
        mlp_gain[None, :],
        jnp.asarray(freqs),
        doc_ids[None, :],
        w_query,
        w_key_value,
        w_out.T,
        w_gate,
        w_up,
        w_down.T,
    )


def solution(mesh):
    every = ("dp", "fsdp")
    in_specs = (
        P(every, None), P(every), P(), P(), P(every, None), P(every, None),
        P(None, every), P(every, None), P(every, None), P(None, every),
    )
    return jax.shard_map(
        per_device, mesh=mesh, in_specs=in_specs, out_specs=P(every, None), check_vma=False
    )
```

```python
import functools
import math

import jax
import jax.numpy as jnp
import numpy as np
from jax import lax
from jax.experimental import pallas as pl
from jax.experimental.pallas import tpu as pltpu
from jax.sharding import PartitionSpec as P

MESH = pl.DeviceIdType.MESH
EPS = 1e-05
THETA = 500000.0
NEGATIVE = -1e30
SIDE = 4
SPAN = 4
GROUPS = (
    ((0, 256, 0), (256, 256, 1), (512, 256, 2)),
    ((768, 256, 0), (1024, 256, 1), (1280, 256, 2)),
    ((1536, 256, 0), (1792, 256, 1), (2048, 256, 2)),
    ((2304, 384, 0), (2688, 256, 1), (2944, 384, 2)),
    ((3328, 128, 0), (3456, 128, 1), (3584, 256, 2)),
    ((3840, 128, 0), (3968, 256, 1), (4224, 128, 2)),
)
ORDERS = (("x", "y", "z"), ("y", "z", "x"), ("z", "x", "y"))
PAIR_AT, QUERY_AT, OUT_AT, DOWN_AT, LAST, WIDTH = 0, 256, 768, 3328, 512, 4352
GATE_AT, UP_AT = (1280, 2304), (1792, 2816)
ARRIVALS = 180


def kernel(
    tok, gain_attn, gain_mlp, freqs, docs, wq, wkv, wo, wg, wu, wd,
    res,
    w, nrm, qry, keys, vals, marks, mine, cosine, sine, power, peaks, sums, mixes, att, hid, acc,
    send, recv, local_sem, tok_sem,
):
    rows, width = res.shape
    heads, _, head = qry.shape
    shard = wq.shape[0]
    half = shard // 2
    dp = lax.axis_index("dp")
    x = lax.axis_index("fsdp")
    y = dp // (2 * SIDE)
    z = (dp // 2) % SIDE
    c = dp % 2
    pos = {"x": x, "y": y, "z": z}
    rank = dp * SIDE + x
    ranks = 32 * SIDE

    def device(at, core):
        return ((at["y"] * SIDE + at["z"]) * 2 + core, at["x"])

    def shift(dim, by):
        return {**pos, dim: (pos[dim] + by) % SIDE}

    def peer(dim, by):
        return device(shift(dim, by), c)

    def at_rank(by):
        other = (rank + by + ranks) % ranks
        return (other // SIDE, other % SIDE)

    local = []
    some = wg.shape[1] // 2
    for src, at in (
        (wkv, PAIR_AT), (wq, QUERY_AT), (wo, OUT_AT), (wd, DOWN_AT),
        (wg.at[:, pl.ds(0, some)], GATE_AT[0]), (wg.at[:, pl.ds(some, some)], GATE_AT[1]),
        (wu.at[:, pl.ds(0, some)], UP_AT[0]), (wu.at[:, pl.ds(some, some)], UP_AT[1]),
    ):
        local.append(
            pltpu.make_async_copy(
                src, w.at[y, z, c, x, :, pl.ds(at, src.shape[1])], local_sem.at[0]
            )
        )
    for copy in local:
        copy.start()
    chunk = rows // 4
    tok_copies = [
        pltpu.make_async_copy(
            tok.at[pl.ds(k * chunk, chunk)], res.at[pl.ds(k * chunk, chunk)], tok_sem.at[k]
        )
        for k in range(4)
    ]
    for copy in tok_copies:
        copy.start()

    barrier = pltpu.get_barrier_semaphore()
    friends = [peer(dim, by) for dim in ("x", "y", "z") for by in (1, 2, 3)]
    friends.append(device(pos, 1 - c))
    friends += [at_rank(by) for by in range(-SPAN, SPAN + 1) if by != 0]
    for friend in friends:
        pl.semaphore_signal(barrier, inc=1, device_id=friend, device_id_type=MESH)
    pl.semaphore_wait(barrier, len(friends))

    arrivals = {}

    def arrival(*key):
        return recv.at[arrivals.setdefault(key, len(arrivals))]

    def block(core, sel, part, r0, nr):
        at, n = part
        return w.at[
            sel["y"], sel["z"], core, sel["x"], pl.ds(r0, nr), pl.ds(at, n)
        ]

    def remote(ref, key, to, sent=0):
        return pltpu.make_async_remote_copy(
            src_ref=ref, dst_ref=ref, send_sem=send.at[sent], recv_sem=arrival(*key),
            device_id=to, device_id_type=MESH,
        )

    def push(ref, key, to, sent):
        remote(ref, key, to, sent).start()

    ALL = slice(None)

    def each(g):
        for p in (2, 0, 1) if g else (0, 2, 1):
            at, n, o = GROUPS[g][p]
            yield g * 3 + p, (at, n), ORDERS[o]

    def keys_of(row, k):
        at = (row, k)
        near_key, far_key = ((*at, 2), (*at, 2)) if k < 2 else ((*at, 2), (*at, 3))
        return (*at, 0), (*at, 1), near_key, far_key

    def spread(row, part, order, k):
        dim = order[k]
        up, down, close, _ = keys_of(row, k)
        sel = {**pos, **{d: ALL for d in order[:k]}}
        push(block(c, sel, part, 0, half), up, peer(dim, 1), k)
        push(block(c, sel, part, half, half), down, peer(dim, -1), k)
        push(block(c, sel, part, half, half), close, peer(dim, 1), k)
        push(block(c, sel, part, 0, half), close, peer(dim, -1), k)

    def downwards(row, order, k):
        return k == 2 and row // 3 in (1, 2) and order[2] != "x"

    def relay(row, part, order, k):
        dim = order[k]
        up, down, close, distant = keys_of(row, k)
        back = {**shift(dim, -1), **{d: ALL for d in order[:k]}}
        ahead = {**shift(dim, 1), **{d: ALL for d in order[:k]}}
        ref = block(c, back, part, 0, half)
        remote(ref, up, peer(dim, 1)).wait_recv()
        if not downwards(row, order, k):
            push(ref, distant, peer(dim, 1), k)
        ref = block(c, ahead, part, half, half)
        remote(ref, down, peer(dim, 1)).wait_recv()
        push(ref, distant, peer(dim, -1), k)
        if downwards(row, order, k):
            whole(row, part, order, k, 1, close)
            push(block(c, ahead, part, 0, half), distant, peer(dim, -1), k)

    def whole(row, part, order, k, blocks, key):
        dim = order[k]
        sel = {**pos, dim: pl.ds(0, blocks), **{d: ALL for d in order[:k]}}
        remote(block(c, sel, part, 0, shard), key, peer(dim, 1)).wait_recv()

    def near(row, part, order, k):
        if not downwards(row, order, k):
            whole(row, part, order, k, 1, keys_of(row, k)[2])

    def far(row, part, order, k):
        whole(row, part, order, k, 1, keys_of(row, k)[3])

    def both(row, part, order, k):
        whole(row, part, order, k, 2, keys_of(row, k)[2])

    def ring(k, what, g, only=None):
        for row, part, order in each(g):
            if only is None or order[2] in only:
                what(row, part, order, k)

    def direct(k, g):
        for row, part, order in each(g):
            sel = {**pos, **{d: ALL for d in order[:k]}}
            for by in (1, 3, 2):
                push(block(c, sel, part, 0, shard), ("direct", k, g), peer(order[k], by), k)

    def span(g):
        lo, hi = GROUPS[g][0], GROUPS[g][-1]
        return pl.ds(lo[0], hi[0] + hi[1] - lo[0])

    def direct_wait(k, g):
        three = pl.ds(0, 3)
        ref = w.at[0, three, 0, ALL, ALL, span(g)] if k else w.at[0, 0, 0, three, ALL, span(g)]
        remote(ref, ("direct", k, g), device(pos, 1 - c)).wait_recv()

    def partner_ref(core, part, order, by):
        sel = {order[0]: ALL, order[1]: ALL, order[2]: (pos[order[2]] + by) % SIDE}
        return block(core, sel, part, 0, shard)

    def shared(row, g):
        return ("share", g, row if g == 0 else 0)

    def share(g, *which):
        for row, part, order in each(g):
            for by in which:
                push(partner_ref(c, part, order, by), shared(row, g), device(pos, 1 - c), 3)

    def share_wait(g, row=0):
        cols = pl.ds(*GROUPS[0][row][:2]) if g == 0 else span(g)
        ref = w.at[ALL, ALL, 1 - c, ALL, ALL, cols]
        remote(ref, shared(row, g), device(pos, 1 - c)).wait_recv()

    def halo(src, dst, slot, by, to):
        key = ("halo", slot, by) if (slot, by) in ((0, 1), (1, 3), (1, 1)) else ("halo", slot)
        return pltpu.make_async_remote_copy(
            src_ref=src, dst_ref=dst, send_sem=send.at[4 + slot], recv_sem=arrival(*key),
            device_id=at_rank(to), device_id_type=MESH,
        )

    def norm(gain, r0, n):
        def step(k, carry):
            at = pl.ds(pl.multiple_of(r0 + k * 16, 16), 16)
            wide = res[at, :].astype(jnp.float32)
            power = jnp.mean(wide * wide, axis=-1, keepdims=True)
            nrm[at, :] = (wide * lax.rsqrt(power + EPS) * gain[...]).astype(jnp.bfloat16)
            return carry

        lax.fori_loop(0, n // 16, step, 0)

    def columns(at, n):
        return w[:, :, :, :, :, pl.ds(at, n)].reshape(width, n)

    def rotated(u):
        return u * cosine[...] + pltpu.roll(u, head // 2, 1) * sine[...]

    scope = jax.named_scope

    def pass_on(src, dst, slot, by, to):
        halo(src, dst, slot, by, to).start()

    def halo_wait(slot, by):
        buf = (keys, vals)[slot]
        halo(buf.at[SPAN], buf.at[SPAN - by], slot, by, by).wait_recv()

    def halo_rest(slot, n):
        ref = (keys, vals, marks)[slot].at[pl.ds(0, n)]
        halo(ref, ref, slot, 4, 4).wait_recv()

    marks[SPAN] = jnp.broadcast_to(docs[...], (8, rows))
    with scope("local"):
        own = w.at[y, z, c, x]
        pltpu.make_async_copy(own, own, local_sem.at[0]).wait()
    direct(0, 0)
    for g in range(1, 6):
        ring(0, spread, g)
    turned = docs[...].astype(jnp.float32)
    mine[...] = jnp.transpose(jnp.broadcast_to(turned, (head, rows))).astype(jnp.int32)
    with scope("norm0"):
        tok_copies[0].wait()
        norm(gain_attn, 0, chunk)
    with scope("B0"):
        direct_wait(0, 0)
        direct(1, 0)
    with scope("Ar"):
        for g in range(1, 6):
            ring(0, relay, g)
    for by in range(1, SPAN + 1):
        pass_on(marks.at[SPAN], marks.at[SPAN - by], 2, by, by)
    with scope("norm1"):
        tok_copies[1].wait()
        norm(gain_attn, chunk, chunk)
    with scope("B1"):
        ring(0, both, 1)
        ring(1, spread, 1)
    with scope("C0"):
        direct_wait(1, 0)
        ring(2, spread, 0)
        share(0, 0)
    with scope("B2"):
        ring(0, both, 2)
        ring(1, spread, 2)
    with scope("norm2"):
        tok_copies[2].wait()
        norm(gain_attn, 2 * chunk, chunk)
    with scope("Br1"):
        ring(1, relay, 1)
    with scope("angles"):
        place = rank * rows + lax.broadcasted_iota(jnp.int32, (rows, head), 0)
        angle = place.astype(jnp.float32) * freqs[...]
        cosine[...] = jnp.cos(angle)
        turn = jnp.sin(angle)
        early = lax.broadcasted_iota(jnp.int32, (rows, head), 1) < head // 2
        sine[...] = jnp.where(early, -turn, turn)
    with scope("Cr0"):
        ring(2, relay, 0)
    with scope("B345"):
        for g in (3, 4, 5):
            ring(0, both, g)
            ring(1, spread, g)
    with scope("norm3"):
        tok_copies[3].wait()
        norm(gain_attn, 3 * chunk, chunk)
    with scope("near0"):
        ring(2, near, 0)
        share(0, 1, 3)
    with scope("Br2"):
        ring(1, relay, 2)
    with scope("C1"):
        ring(1, both, 1)
        ring(2, spread, 1)
    with scope("far0"):
        for row, part, order in each(0):
            far(row, part, order, 2)
            push(partner_ref(c, part, order, 2), shared(row, 0), device(pos, 1 - c), 3)
    with scope("F0"):
        share_wait(0, 0)

    with scope("pair"):
        pair = jnp.dot(nrm[...], columns(PAIR_AT, 256), preferred_element_type=jnp.float32)
        keys[SPAN] = jnp.transpose(rotated(pair[:, :head])).astype(jnp.bfloat16)
        vals[SPAN] = pair[:, head:].astype(jnp.bfloat16)
    with scope("Br345"):
        for g in (3, 4, 5):
            ring(1, relay, g)
    pass_on(keys.at[SPAN], keys.at[SPAN - 1], 0, 1, 1)
    pass_on(vals.at[SPAN], vals.at[SPAN - 3], 1, 3, 3)
    pass_on(vals.at[SPAN], vals.at[SPAN - 1], 1, 1, 1)
    pass_on(keys.at[SPAN], keys.at[SPAN - 3], 0, 3, 3)
    pass_on(keys.at[SPAN], keys.at[SPAN - 4], 0, 4, 4)
    pass_on(vals.at[SPAN], vals.at[SPAN - 4], 1, 4, 4)
    with scope("query"):
        share_wait(0, 1)
        share_wait(0, 2)
        for p in range(2):
            raw = jnp.dot(nrm[...], columns(QUERY_AT + 256 * p, 256), preferred_element_type=jnp.float32)
            for k in range(2):
                qry[2 * p + k] = rotated(raw[:, k * head : (k + 1) * head]).astype(jnp.bfloat16)
    share(1, 0)

    def begin_last(g, along):
        ring(1, both, g, along)
        ring(2, spread, g, along)

    def advance(g, along):
        for dim in along:
            ring(2, relay, g, dim)
            begin_last(g + 2, dim)

    with scope("Cr1"):
        ring(2, relay, 1)
    with scope("C2yz"):
        ring(1, both, 2, "yz")
        ring(2, spread, 2, "yz")
    with scope("forward"):
        halo_wait(0, 1)
        pass_on(keys.at[SPAN - 1], keys.at[SPAN - 2], 0, 2, 1)
        halo_wait(1, 3)
        pass_on(vals.at[SPAN - 3], vals.at[SPAN - 2], 1, 2, -1)
    tall = rows // 2
    scale = math.log2(math.e) / math.sqrt(head)

    def scored(part, h, spans):
        q = qry[h, part * tall : (part + 1) * tall, :]
        own = mine[part * tall : (part + 1) * tall, 0:1]
        scores = []
        for j, at, n, causal in spans:
            s = jnp.dot(q, keys[j, :, at : at + n], preferred_element_type=jnp.float32)
            same = marks[j, 0:1, at : at + n] == own
            if causal:
                same = same & (
                    lax.broadcasted_iota(jnp.int32, (tall, n), 1)
                    <= lax.broadcasted_iota(jnp.int32, (tall, n), 0)
                )
            scores.append(jnp.where(same, s, NEGATIVE))
        peak = functools.reduce(
            jnp.maximum, [jnp.max(s, axis=1, keepdims=True) for s in scores]
        )
        return scores, peak

    def weighed(spans, scores, peak, total, mixed):
        for (j, at, n, _), s in zip(spans, scores):
            e = jnp.exp2((s - peak) * scale)
            total = total + jnp.sum(e, axis=1, keepdims=True)
            mixed = mixed + jnp.dot(
                e.astype(jnp.bfloat16), vals[j, at : at + n, :], preferred_element_type=jnp.float32
            )
        return total, mixed

    def attend_near(part, h):
        here = pl.ds(part * tall, tall)
        spans = [(SPAN, part * tall, tall, True)]
        if part == 1:
            spans.append((SPAN, 0, tall, False))
        spans.append((SPAN - 1, 0, rows, False))
        scores, peak = scored(part, h, spans)
        total = jnp.zeros((tall, 1), jnp.float32)
        mixed = jnp.zeros((tall, head), jnp.float32)
        total, mixed = weighed(spans, scores, peak, total, mixed)
        peaks[h, here, :] = jnp.broadcast_to(peak, (tall, head))
        sums[h, here, :] = jnp.broadcast_to(total, (tall, head))
        mixes[h, here, :] = mixed

    def attend_far(part, h):
        here = pl.ds(part * tall, tall)
        spans = [(0, tall * part, rows - tall * part, False)]
        spans += [(j, 0, rows, False) for j in range(1, SPAN - 1)]
        scores, peak = scored(part, h, spans)
        old = peaks[h, here, 0:1]
        peak = jnp.maximum(peak, old)
        factor = jnp.exp2((old - peak) * scale)
        total = sums[h, here, 0:1] * factor
        mixed = mixes[h, here, :] * factor
        total, mixed = weighed(spans, scores, peak, total, mixed)
        att[here, pl.ds(pl.multiple_of(h * head, head), head)] = (mixed / total).astype(jnp.bfloat16)

    def attend_heads(what, part, lo, hi):
        def step(h, carry):
            what(part, h)
            return carry

        lax.fori_loop(lo, hi, step, 0)

    with scope("C2x"):
        begin_last(2, "x")
    with scope("C3"):
        begin_last(3, "yzx")
    with scope("near1"):
        ring(2, near, 1)
        share(1, 1, 3)
    with scope("early0"):
        halo_rest(2, 4)
        halo_wait(1, 1)
        attend_heads(attend_near, 0, 0, heads)
    with scope("early1"):
        attend_heads(attend_near, 1, 0, heads)
    with scope("Cr2y"):
        advance(2, "y")
    with scope("far1"):
        ring(2, far, 1)
        share(1, 2)
    with scope("halo"):
        halo_rest(0, 3)
        halo_rest(1, 2)
    with scope("attend0"):
        attend_heads(attend_far, 0, 0, 2)
    with scope("Cr2zx"):
        advance(2, "zx")

    share(2, 0)
    with scope("attend1"):
        attend_heads(attend_far, 0, 2, 4)
    with scope("Cr3y"):
        advance(3, "y")
    with scope("attend2"):
        attend_heads(attend_far, 1, 0, 2)
    with scope("near2"):
        ring(2, near, 2)
        share(2, 1, 3)
    with scope("attend3"):
        attend_heads(attend_far, 1, 2, 4)
    share(3, 0)
    with scope("Cr3xz"):
        advance(3, "xz")
    with scope("F1"):
        share_wait(1)

    def wide_step(lhs, lo, n, at, use):
        per = 2 * 2 * SIDE * shard

        def step(k, carry):
            for zz in range(2):
                rhs = w[k, 2 * zz : 2 * zz + 2, :, :, :, at : at + n].reshape(per, n)
                got = lax.dot_general(
                    lhs[:, lo : lo + n], rhs, (((1,), (1,)), ((), ())), preferred_element_type=jnp.float32
                )
                use(pl.ds(pl.multiple_of((k * 2 + zz) * per, per), per), got)
            return carry

        lax.fori_loop(0, SIDE, step, 0)

    def project(here, got):
        new = (res[:, here].astype(jnp.float32) + got).astype(jnp.bfloat16)
        res[:, here] = new
        wide = new.astype(jnp.float32)
        wide = wide * wide
        parts = [wide[:, i * head : (i + 1) * head] for i in range(got.shape[1] // head)]
        power[...] += functools.reduce(jnp.add, parts)

    def begin(here, got):
        acc[:, here] = res[:, here].astype(jnp.float32) + got

    def end(here, got):
        res[:, here] = (acc[:, here] + got).astype(jnp.bfloat16)

    def scaled(gain):
        mean = jnp.sum(power[...], axis=-1, keepdims=True) / width
        power[...] = jnp.broadcast_to(lax.rsqrt(mean + EPS), (rows, head))

        def step(k, carry):
            at = pl.ds(pl.multiple_of(k * 32, 32), 32)
            inverse = power[at, :]
            for i in range(width // head):
                lanes = slice(i * head, (i + 1) * head)
                wide = res[at, lanes].astype(jnp.float32)
                nrm[at, lanes] = (wide * inverse * gain[:, lanes]).astype(jnp.bfloat16)
            return carry

        lax.fori_loop(0, rows // 32, step, 0)

    power[...] = jnp.zeros_like(power)
    with scope("project"):
        wide_step(att, 0, heads * head, OUT_AT, project)
    with scope("far2"):
        ring(2, far, 2)
        share(2, 2)
    with scope("mlp_norm"):
        scaled(gain_mlp)
    with scope("F2"):
        share_wait(2)

    def gated(part, j):
        at = 256 * j
        gate = jnp.dot(nrm[...], columns(GATE_AT[part] + at, 256), preferred_element_type=jnp.float32)
        up = jnp.dot(nrm[...], columns(UP_AT[part] + at, 256), preferred_element_type=jnp.float32)
        here = part * some + at
        hid[:, here : here + 256] = (gate / (1.0 + jnp.exp(-gate)) * up).astype(jnp.bfloat16)

    with scope("Cr4"):
        ring(2, relay, 4)
    with scope("near3"):
        ring(2, near, 3)
        share(3, 1, 3)
    with scope("gated0"):
        gated(0, 0)
    with scope("gated1"):
        gated(0, 1)
    with scope("far3"):
        ring(2, far, 3)
        share(3, 2)
        share(4, 0)
    with scope("F3"):
        share_wait(3)
    with scope("near4"):
        ring(2, near, 4)
        share(4, 1, 3)
    with scope("Cr5"):
        ring(2, relay, 5)
    with scope("gated2"):
        gated(1, 0)
    with scope("far4"):
        ring(2, far, 4)
        share(4, 2)
        share(5, 0)
    with scope("gated3"):
        gated(1, 1)
    with scope("near5"):
        ring(2, near, 5)
        share(5, 1, 3)
    with scope("far5"):
        ring(2, far, 5)
        share(5, 2)
    with scope("F4"):
        share_wait(4)
    with scope("down0"):
        wide_step(hid, 0, LAST, DOWN_AT, begin)
    with scope("F5"):
        share_wait(5)
    with scope("down1"):
        wide_step(hid, LAST, hid.shape[1] - LAST, DOWN_AT + LAST, end)
    assert len(arrivals) <= ARRIVALS
    with scope("sent"):
        three = pl.ds(0, 3)
        for k, ref in enumerate(
            (w.at[0, 0, 0, three], w.at[0, three, 0], w.at[three, ALL, 0], w.at[ALL, ALL, 0])
        ):
            remote(ref, shared(0, 1), device(pos, 1 - c), k).wait_send()
        for slot, buf in enumerate((keys, vals, marks)):
            ref = buf.at[pl.ds(0, 4)]
            halo(ref, ref, slot, 4, 4).wait_send()


def per_device(
    tokens, doc_ids, attn_gain, mlp_gain, w_query, w_key_value, w_out, w_gate, w_up, w_down
):
    rows, width = tokens.shape
    head = w_key_value.shape[1] // 2
    heads = w_query.shape[1] // head
    shard = w_query.shape[0]
    freqs = THETA ** (-2.0 * np.arange(head // 2) / head)
    freqs = np.concatenate([freqs, freqs])[None, :].astype(np.float32)
    vmem = pl.BlockSpec(memory_space=pltpu.VMEM)
    anywhere = pl.BlockSpec(memory_space=pl.ANY)
    bf16 = jnp.bfloat16
    return pl.pallas_call(
        kernel,
        out_shape=pltpu.VMEM((rows, width), bf16),
        in_specs=[anywhere] + [vmem] * 4 + [anywhere] * 6,
        out_specs=vmem,
        scratch_shapes=[
            pltpu.VMEM((SIDE, SIDE, 2, SIDE, shard, WIDTH), bf16),
            pltpu.VMEM((rows, width), bf16),
            pltpu.VMEM((heads, rows, head), bf16),
            pltpu.VMEM((SPAN + 1, head, rows), bf16),
            pltpu.VMEM((SPAN + 1, rows, head), bf16),
            pltpu.VMEM((SPAN + 1, 8, rows), jnp.int32),
            pltpu.VMEM((rows, head), jnp.int32),
            pltpu.VMEM((rows, head), jnp.float32),
            pltpu.VMEM((rows, head), jnp.float32),
            pltpu.VMEM((rows, head), jnp.float32),
            pltpu.VMEM((heads, rows, head), jnp.float32),
            pltpu.VMEM((heads, rows, head), jnp.float32),
            pltpu.VMEM((heads, rows, head), jnp.float32),
            pltpu.VMEM((rows, heads * head), bf16),
            pltpu.VMEM((rows, w_gate.shape[1]), bf16),
            pltpu.VMEM((rows, width), jnp.float32),
            pltpu.SemaphoreType.DMA((7,)),
            pltpu.SemaphoreType.DMA((ARRIVALS,)),
            pltpu.SemaphoreType.DMA((1,)),
            pltpu.SemaphoreType.DMA((4,)),
        ],
        compiler_params=pltpu.CompilerParams(
            collective_id=0, has_side_effects=True, vmem_limit_bytes=58 * 1024 * 1024
        ),
    )(
        tokens,
        attn_gain[None, :],
        mlp_gain[None, :],
        jnp.asarray(freqs),
        doc_ids[None, :],
        w_query,
        w_key_value,
        w_out.T,
        w_gate,
        w_up,
        w_down.T,
    )


def solution(mesh):
    every = ("dp", "fsdp")
    in_specs = (
        P(every, None), P(every), P(), P(), P(every, None), P(every, None),
        P(None, every), P(every, None), P(every, None), P(None, every),
    )
    return jax.shard_map(
        per_device, mesh=mesh, in_specs=in_specs, out_specs=P(every, None), check_vma=False
    )
```
